32 devices in a mesh: gx: 4 (over y, x), gy: 2 (over core), gz: 4 (over z).
Axes of the slice: x: 2, y: 2, z: 4, core: 2. Of those that a mesh axis runs over, the one named last changes fastest.
Arguments:
- initial: float32 [256, 64, 1024], P('gx', 'gy', 'gz'), may hold values from -6 to 6
- right_side: float32 [256, 64, 1024], P('gx', 'gy', 'gz'), may hold values from -12 to 12
- shift_field: float32 [256, 64, 1024], P('gx', 'gy', 'gz'), may hold values from 0.5 to 8
Outputs:
- relaxed: float32 [256, 64, 1024], P('gx', 'gy', 'gz')
The draws below stay inside these ranges and needn't reach their ends.
All inputs are finite; a program needn't handle non-finite values.
Results may differ from the reference program's by a relative error of at most 0.00002.
Values sent between devices are 32-bit elements; how exact they have to be, the bound alone decides.
A program may use at most 128 MiB of HBM per device.

```python
import math
import jax
import jax.numpy as jnp

SWEEPS = 4
NX = 256
NY = 64
NZ = 1024


def levels(stream_key, extent, cuts, least, high):
    def one(position, parts):
        heights = jax.random.uniform(jax.random.fold_in(jax.random.fold_in(stream_key, 6), position), (parts,), jnp.float32, least / len(cuts), high / len(cuts))
        return jnp.repeat(jnp.exp(heights), extent[position] // parts).reshape((-1,) + (1,) * (len(extent) - position - 1))

    gain = one(*cuts[0])
    for cut in cuts[1:]:
        gain = gain * one(*cut)
    return gain


def centred(stream_key, extent, scale, limit, pieces=(), held_as=jnp.bfloat16):
    array = scale * jax.random.normal(stream_key, extent, jnp.float32)
    if pieces:
        array = array * levels(stream_key, extent, pieces, -0.22, 0.18)
    return jnp.clip(array, -limit, limit).astype(held_as)


def setup_inputs(seed: int = 0) -> dict:
    keys = jax.random.split(jax.random.key(seed), 4)
    initial = centred(keys[0], (NX, NY, NZ), 1.0, 6.0, ((0, 4), (1, 2), (2, 4)), jnp.float32)
    right_side = centred(keys[1], (NX, NY, NZ), 2.0, 12.0, ((0, 4), (1, 2), (2, 4)), jnp.float32)
    shift_field = jnp.clip(jnp.exp(math.log(8.0) - 2.7725887 * jax.random.uniform(keys[2], (NX, NY, NZ), jnp.float32) ** levels(keys[2], (NX, NY, NZ), ((0, 4), (1, 2), (2, 4)), -0.2, 0.2)), 0.5, 8.0)
    return dict(initial=initial, right_side=right_side, shift_field=shift_field)


relax_weight = 0.8


def neighbours(field):
    total = jnp.roll(field, 1, 0) + jnp.roll(field, -1, 0)
    total = total + jnp.roll(field, 1, 1) + jnp.roll(field, -1, 1)
    total = total + jnp.roll(field, 1, 2) + jnp.roll(field, -1, 2)
    return total


def reference(initial, right_side, shift_field):
    diagonal = 6.0 + shift_field
    relaxed = initial
    for sweep in range(SWEEPS):
        beside = neighbours(relaxed)
        relaxed = relaxed + relax_weight * (right_side - (diagonal * relaxed - beside)) / diagonal
    return relaxed
```

```python
import functools

import jax
import jax.numpy as jnp
import numpy as np
from jax import lax
from jax.experimental import pallas as pl
from jax.experimental.pallas import tpu as pltpu
from jax.sharding import PartitionSpec as P

SWEEPS = 4
WEIGHT = np.float32(0.8)
KEEP = np.float32(1.0) - WEIGHT
AXES = ("gx", "gy", "gz")
MESH = pl.DeviceIdType.MESH
ROWS = 8
LANES = 128
GROUP = 16
PREPARED = 8
CHUNKS = 4


def beside(axis, step):
    count = lax.axis_size(axis)
    return {axis: lax.rem(lax.axis_index(axis) + (count + step), count)}


def iota(dim, shape):
    return lax.broadcasted_iota(jnp.int32, shape, dim)


def turned(block, shift, dim):
    size = block.shape[dim]
    shift = shift % size
    return block if shift == 0 else pltpu.roll(block, shift, dim)


def kernel(init_ref, rhs_ref, shift_ref, out_ref, v, q, w, z, zh, load, send, recv):
    nx, ny, nz = out_ref.shape
    groups, bands, tiles = nx // GROUP, ny // ROWS, nz // LANES
    per = nx // CHUNKS

    barrier = pltpu.get_barrier_semaphore()
    for axis in AXES:
        for step in (-1, 1):
            pl.semaphore_signal(barrier, inc=1, device_id=beside(axis, step), device_id_type=MESH)

    def part(array, j):
        return array.at[:, :, pl.ds(LANES * j, LANES)]

    def init_copies(c):
        return [
            pltpu.make_async_copy(
                init_ref.at[pl.ds(c * per, per), :, pl.ds(LANES * j, LANES)],
                v.at[0, pl.ds(c * per + 1, per), j, pl.ds(ROWS, ny)],
                load.at[c * tiles + j],
            )
            for j in range(tiles)
        ]

    def field_copies(array, held, slot):
        return [
            pltpu.make_async_copy(part(array, j), held.at[:, j], load.at[(CHUNKS + slot) * tiles + j])
            for j in range(tiles)
        ]

    def start(copies):
        for copy in copies:
            copy.start()

    def wait(copies):
        for copy in copies:
            copy.wait()

    for c in range(CHUNKS):
        start(init_copies(c))
    field_loads = field_copies(shift_ref, w, 0) + field_copies(rhs_ref, q, 1)
    start(field_loads)

    def remote(src, dst, t, face, axis, step):
        return pltpu.make_async_remote_copy(
            src_ref=src,
            dst_ref=dst,
            send_sem=send.at[t, face],
            recv_sem=recv.at[t, face],
            device_id=beside(axis, step),
            device_id_type=MESH,
        )

    def x_copies(t):
        def plane(x):
            return v.at[t, x + 1, :, pl.ds(ROWS, ny)]

        return (
            remote(plane(nx - 1), plane(-1), t, 0, "gx", 1),
            remote(plane(0), plane(nx), t, 1, "gx", -1),
        )

    def y_copies(t):
        def row(y):
            return v.at[t, pl.ds(1, nx), :, pl.ds(ROWS + y, 1)]

        return (
            remote(row(ny - 1), row(-1), t, 2, "gy", 1),
            remote(row(0), row(ny), t, 3, "gy", -1),
        )

    def z_copies(t):
        return (
            remote(z.at[t], zh.at[t, 0], t, 4, "gz", 1),
            remote(z.at[t], zh.at[t, 1], t, 5, "gz", -1),
        )

    lane = iota(1, (ROWS, LANES))
    first_lane = lane == 0
    last_lane = lane == LANES - 1
    blank = jnp.zeros((ROWS, LANES), jnp.float32)

    def rows(k, shift=0):
        return slice(ROWS + ROWS * k + shift, 2 * ROWS + ROWS * k + shift)

    def spots(x):
        return (lane == 2 * x % LANES) | (lane == (2 * x - 1) % LANES)

    def ends(low, high):
        return jnp.where(first_lane, low, high)

    def packed(held, x, low, high):
        return jnp.where(spots(x), turned(ends(low, high), 2 * x, 1), held)

    def put(t, x, j, k, new):
        if t < SWEEPS:
            v[t, x + 1, j, rows(k)] = new
        else:
            out_ref[x, ROWS * k : ROWS * k + ROWS, LANES * j : LANES * j + LANES] = new

    def get(t, x, j, k):
        if t < SWEEPS:
            return v[t, x + 1, j, rows(k)]
        return out_ref[x, ROWS * k : ROWS * k + ROWS, LANES * j : LANES * j + LANES]

    def put_lane(t, x, j, k, new, mask):
        if t < SWEEPS:
            pltpu.store(v.at[t, x + 1, j, pl.ds(ROWS + ROWS * k, ROWS)], new, mask=mask)
        else:
            pltpu.store(
                out_ref.at[x, pl.ds(ROWS * k, ROWS), pl.ds(LANES * j, LANES)], new, mask=mask
            )

    def packed_all(low, high, planes=None):
        held = [blank] * bands
        for x in range(nx) if planes is None else planes:
            for k in range(bands):
                held[k] = packed(held[k], x, low(x, k), high(x, k))
        return held

    for c in range(CHUNKS):
        wait(init_copies(c))
    face = packed_all(lambda x, k: v[0, x + 1, 0, rows(k)], lambda x, k: v[0, x + 1, tiles - 1, rows(k)])
    for k in range(bands):
        z[0, ROWS * k : ROWS * k + ROWS] = face[k]

    pl.semaphore_wait(barrier, 2 * len(AXES))
    start(z_copies(0) + x_copies(0) + y_copies(0))

    wait(field_loads)

    def prepare(g, carry):
        for i in range(PREPARED):
            x = g * PREPARED + i
            for k in range(bands):
                at = slice(ROWS * k, ROWS * k + ROWS)
                for j in range(tiles):
                    ratio = WEIGHT / (6.0 + w[x, j, at])
                    w[x, j, at] = ratio
                    q[x, j, at] = ratio * q[x, j, at]
        return carry

    lax.fori_loop(0, nx // PREPARED, prepare, 0)
    wz = packed_all(
        lambda x, k: w[x, 0, ROWS * k : ROWS * k + ROWS], lambda x, k: w[x, tiles - 1, ROWS * k : ROWS * k + ROWS]
    )

    def bulk_group(t, g, carry):
        base = g * GROUP
        seen = {}

        def plane(i):
            if i not in seen:
                x = base + i
                if i < 0:
                    x = jnp.maximum(x, 0)
                if i == GROUP:
                    x = jnp.minimum(x, nx - 1)
                seen[i] = [[v[t, x + 1, j, rows(k)] for k in range(bands)] for j in range(tiles)]
                if i < 0:
                    inside = jnp.where(g > 0, 1.0, 0.0)
                    seen[i] = [[inside * cell for cell in column] for column in seen[i]]
                if i == GROUP:
                    inside = jnp.where(g < groups - 1, 1.0, 0.0)
                    seen[i] = [[inside * cell for cell in column] for column in seen[i]]
            return seen[i]

        for i in range(GROUP):
            x = base + i
            centre, below, above = plane(i), plane(i - 1), plane(i + 1)
            for k in range(bands):
                at = slice(ROWS * k, ROWS * k + ROWS)
                before = [turned(centre[j][k], 1, 1) for j in range(tiles)]
                after = [turned(centre[j][k], -1, 1) for j in range(tiles)]
                for j in range(tiles):
                    total = v[t, x + 1, j, rows(k, -1)] + v[t, x + 1, j, rows(k, 1)]
                    total = total + (below[j][k] + above[j][k])
                    low = before[j - 1] if j else 0.0
                    high = after[j + 1] if j + 1 < tiles else 0.0
                    total = total + (
                        jnp.where(first_lane, low, before[j]) + jnp.where(last_lane, high, after[j])
                    )
                    put(t + 1, x, j, k, (KEEP * centre[j][k] + q[x, j, at]) + w[x, j, at] * total)
        return carry

    def bulk(t):
        lax.fori_loop(0, groups, functools.partial(bulk_group, t), 0)

    def mend(t, faces):
        for x in range(1, nx - 1):
            for k in range(bands):
                value = turned(faces[k], -2 * x, 1)
                put_lane(t, x, 0, k, value, first_lane)
                put_lane(t, x, tiles - 1, k, value, last_lane)

    even = lane % 2 == 0
    edges = ((0, -1), (nx - 1, nx))
    for t in range(SWEEPS):
        wait(y_copies(t))
        bulk(t)
        partial = packed_all(
            lambda x, k: get(t + 1, x, 0, k), lambda x, k: get(t + 1, x, tiles - 1, k), range(1, nx - 1)
        )
        wait(x_copies(t) + z_copies(t))
        planes = []
        for x, outside in edges:
            plane = [
                [
                    get(t + 1, x, j, k)
                    + w[x, j, ROWS * k : ROWS * k + ROWS] * v[t, outside + 1, j, rows(k)]
                    for k in range(bands)
                ]
                for j in range(tiles)
            ]
            for k in range(bands):
                partial[k] = packed(partial[k], x, plane[0][k], plane[-1][k])
            planes.append(plane)
        faces = []
        for k in range(bands):
            at = slice(ROWS * k, ROWS * k + ROWS)
            halo = jnp.where(even, turned(zh[t, 0, at], 1, 1), turned(zh[t, 1, at], -1, 1))
            faces.append(partial[k] + wz[k] * halo)
            if t + 1 < SWEEPS:
                z[t + 1, at] = faces[k]
        if t + 1 < SWEEPS:
            start(z_copies(t + 1))
        for (x, _), plane in zip(edges, planes):
            for k in range(bands):
                value = turned(faces[k], -2 * x, 1)
                plane[0][k] = jnp.where(first_lane, value, plane[0][k])
                plane[-1][k] = jnp.where(last_lane, value, plane[-1][k])
                for j in range(tiles):
                    put(t + 1, x, j, k, plane[j][k])
        if t + 1 < SWEEPS:
            start(x_copies(t + 1))
        mend(t + 1, faces)
        if t + 1 < SWEEPS:
            start(y_copies(t + 1))


def shards(initial, right_side, shift_field):
    nx, ny, nz = initial.shape
    assert nx % GROUP == 0 and nx % PREPARED == 0 and nx % CHUNKS == 0 and 2 * nx <= LANES
    assert ny % ROWS == 0 and nz % LANES == 0
    faces, tiles = 2 * len(AXES), nz // LANES
    return pl.pallas_call(
        kernel,
        out_shape=pltpu.VMEM((nx, ny, nz), jnp.float32),
        in_specs=[pl.BlockSpec(memory_space=pltpu.HBM)] * 3,
        out_specs=pl.BlockSpec(memory_space=pltpu.VMEM),
        scratch_shapes=[
            pltpu.VMEM((SWEEPS, nx + 2, tiles, ny + 2 * ROWS, LANES), jnp.float32),
            pltpu.VMEM((nx, tiles, ny, LANES), jnp.float32),
            pltpu.VMEM((nx, tiles, ny, LANES), jnp.float32),
            pltpu.VMEM((SWEEPS, ny, LANES), jnp.float32),
            pltpu.VMEM((SWEEPS, 2, ny, LANES), jnp.float32),
            pltpu.SemaphoreType.DMA(((CHUNKS + 2) * tiles,)),
            pltpu.SemaphoreType.DMA((SWEEPS, faces)),
            pltpu.SemaphoreType.DMA((SWEEPS, faces)),
        ],
        compiler_params=pltpu.CompilerParams(
            collective_id=0, has_side_effects=True, vmem_limit_bytes=40 * 1024 * 1024
        ),
    )(*(pltpu.with_memory_space_constraint(a, pltpu.HBM) for a in (initial, right_side, shift_field)))


def solution(mesh):
    spec = P(*AXES)
    return jax.shard_map(
        shards, mesh=mesh, in_specs=(spec, spec, spec), out_specs=spec, check_vma=False
    )
```

```python
import functools

import jax
import jax.numpy as jnp
import numpy as np
from jax import lax
from jax.experimental import pallas as pl
from jax.experimental.pallas import tpu as pltpu
from jax.sharding import PartitionSpec as P

SWEEPS = 4
WEIGHT = np.float32(0.8)
KEEP = np.float32(1.0) - WEIGHT
AXES = ("gx", "gy", "gz")
MESH = pl.DeviceIdType.MESH
ROWS = 8
LANES = 128
GROUP = 16
PREPARED = 8
CHUNKS = 4


def beside(axis, step):
    count = lax.axis_size(axis)
    return {axis: lax.rem(lax.axis_index(axis) + (count + step), count)}


def iota(dim, shape):
    return lax.broadcasted_iota(jnp.int32, shape, dim)


def turned(block, shift, dim):
    size = block.shape[dim]
    shift = shift % size
    return block if shift == 0 else pltpu.roll(block, shift, dim)


def kernel(init_ref, rhs_ref, shift_ref, out_ref, v, q, w, z, zh, load, send, recv):
    nx, ny, nz = out_ref.shape
    groups, bands, tiles = nx // GROUP, ny // ROWS, nz // LANES
    per = nx // CHUNKS

    barrier = pltpu.get_barrier_semaphore()
    for axis in AXES:
        for step in (-1, 1):
            pl.semaphore_signal(barrier, inc=1, device_id=beside(axis, step), device_id_type=MESH)

    def part(array, j):
        return array.at[:, :, pl.ds(LANES * j, LANES)]

    def init_copies(c):
        return [
            pltpu.make_async_copy(
                init_ref.at[pl.ds(c * per, per), :, pl.ds(LANES * j, LANES)],
                v.at[0, pl.ds(c * per + 1, per), j, pl.ds(ROWS, ny)],
                load.at[c * tiles + j],
            )
            for j in range(tiles)
        ]

    def field_copies(array, held, slot):
        return [
            pltpu.make_async_copy(part(array, j), held.at[:, j], load.at[(CHUNKS + slot) * tiles + j])
            for j in range(tiles)
        ]

    def start(copies):
        for copy in copies:
            copy.start()

    def wait(copies):
        for copy in copies:
            copy.wait()

    for c in range(CHUNKS):
        start(init_copies(c))
    field_loads = field_copies(shift_ref, w, 0) + field_copies(rhs_ref, q, 1)
    start(field_loads)

    def remote(src, dst, t, face, axis, step):
        return pltpu.make_async_remote_copy(
            src_ref=src,
            dst_ref=dst,
            send_sem=send.at[t, face],
            recv_sem=recv.at[t, face],
            device_id=beside(axis, step),
            device_id_type=MESH,
        )

    def x_copies(t):
        def plane(x):
            return v.at[t, x + 1, :, pl.ds(ROWS, ny)]

        return (
            remote(plane(nx - 1), plane(-1), t, 0, "gx", 1),
            remote(plane(0), plane(nx), t, 1, "gx", -1),
        )

    def y_copies(t):
        def row(y):
            return v.at[t, pl.ds(1, nx), :, pl.ds(ROWS + y, 1)]

        return (
            remote(row(ny - 1), row(-1), t, 2, "gy", 1),
            remote(row(0), row(ny), t, 3, "gy", -1),
        )

    def z_copies(t):
        return (
            remote(z.at[t, 1], zh.at[t, 0], t, 4, "gz", 1),
            remote(z.at[t, 0], zh.at[t, 1], t, 5, "gz", -1),
        )

    lane = iota(1, (ROWS, LANES))
    first_lane = lane == 0
    last_lane = lane == LANES - 1
    blank = jnp.zeros((ROWS, LANES), jnp.float32)

    def rows(k, shift=0):
        return slice(ROWS + ROWS * k + shift, 2 * ROWS + ROWS * k + shift)

    def spots(x, k):
        return (lane == (2 * x + k % 2) % LANES) | (lane == (2 * x + k % 2 - 1) % LANES)

    def packed(held, x, k, low, high):
        ends = jnp.where(first_lane, low, high)
        return jnp.where(spots(x, k), turned(ends, 2 * x + k % 2, 1), held)

    even = lane % 2 == 0

    def ship(t, faces):
        for m in range(bands // 2):
            at = slice(ROWS * m, ROWS * m + ROWS)
            z[t, 0, at] = jnp.where(even, faces[2 * m], faces[2 * m + 1])
            z[t, 1, at] = jnp.where(even, faces[2 * m + 1], faces[2 * m])

    def put(t, x, j, k, new):
        if t < SWEEPS:
            v[t, x + 1, j, rows(k)] = new
        else:
            out_ref[x, ROWS * k : ROWS * k + ROWS, LANES * j : LANES * j + LANES] = new

    def get(t, x, j, k):
        if t < SWEEPS:
            return v[t, x + 1, j, rows(k)]
        return out_ref[x, ROWS * k : ROWS * k + ROWS, LANES * j : LANES * j + LANES]

    def put_lane(t, x, j, k, new, mask):
        if t < SWEEPS:
            pltpu.store(v.at[t, x + 1, j, pl.ds(ROWS + ROWS * k, ROWS)], new, mask=mask)
        else:
            pltpu.store(
                out_ref.at[x, pl.ds(ROWS * k, ROWS), pl.ds(LANES * j, LANES)], new, mask=mask
            )

    def packed_all(low, high, planes=None):
        held = [blank] * bands
        for x in range(nx) if planes is None else planes:
            for k in range(bands):
                held[k] = packed(held[k], x, k, low(x, k), high(x, k))
        return held

    for c in range(CHUNKS):
        wait(init_copies(c))
    face = packed_all(lambda x, k: v[0, x + 1, 0, rows(k)], lambda x, k: v[0, x + 1, tiles - 1, rows(k)])
    ship(0, face)

    pl.semaphore_wait(barrier, 2 * len(AXES))
    start(z_copies(0) + x_copies(0) + y_copies(0))

    wait(field_loads)

    def prepare(g, carry):
        for i in range(PREPARED):
            x = g * PREPARED + i
            for k in range(bands):
                at = slice(ROWS * k, ROWS * k + ROWS)
                for j in range(tiles):
                    ratio = WEIGHT / (6.0 + w[x, j, at])
                    w[x, j, at] = ratio
                    q[x, j, at] = ratio * q[x, j, at]
        return carry

    lax.fori_loop(0, nx // PREPARED, prepare, 0)
    wz = packed_all(
        lambda x, k: w[x, 0, ROWS * k : ROWS * k + ROWS], lambda x, k: w[x, tiles - 1, ROWS * k : ROWS * k + ROWS]
    )

    def bulk_group(t, g, carry):
        base = g * GROUP
        seen = {}

        def plane(i):
            if i not in seen:
                x = base + i
                if i < 0:
                    x = jnp.maximum(x, 0)
                if i == GROUP:
                    x = jnp.minimum(x, nx - 1)
                seen[i] = [[v[t, x + 1, j, rows(k)] for k in range(bands)] for j in range(tiles)]
                if i < 0:
                    inside = jnp.where(g > 0, 1.0, 0.0)
                    seen[i] = [[inside * cell for cell in column] for column in seen[i]]
                if i == GROUP:
                    inside = jnp.where(g < groups - 1, 1.0, 0.0)
                    seen[i] = [[inside * cell for cell in column] for column in seen[i]]
            return seen[i]

        for i in range(GROUP):
            x = base + i
            centre, below, above = plane(i), plane(i - 1), plane(i + 1)
            for k in range(bands):
                at = slice(ROWS * k, ROWS * k + ROWS)
                before = [turned(centre[j][k], 1, 1) for j in range(tiles)]
                after = [turned(centre[j][k], -1, 1) for j in range(tiles)]
                for j in range(tiles):
                    total = v[t, x + 1, j, rows(k, -1)] + v[t, x + 1, j, rows(k, 1)]
                    total = total + (below[j][k] + above[j][k])
                    low = before[j - 1] if j else 0.0
                    high = after[j + 1] if j + 1 < tiles else 0.0
                    total = total + (
                        jnp.where(first_lane, low, before[j]) + jnp.where(last_lane, high, after[j])
                    )
                    put(t + 1, x, j, k, (KEEP * centre[j][k] + q[x, j, at]) + w[x, j, at] * total)
        return carry

    def bulk(t):
        lax.fori_loop(0, groups, functools.partial(bulk_group, t), 0)

    def mend(t, faces):
        for x in range(1, nx - 1):
            for k in range(bands):
                value = turned(faces[k], -2 * x - k % 2, 1)
                put_lane(t, x, 0, k, value, first_lane)
                put_lane(t, x, tiles - 1, k, value, last_lane)

    edges = ((0, -1), (nx - 1, nx))
    for t in range(SWEEPS):
        wait(y_copies(t))
        bulk(t)
        partial = packed_all(lambda x, k: get(t + 1, x, 0, k), lambda x, k: get(t + 1, x, tiles - 1, k))
        wait(x_copies(t) + z_copies(t))
        from_low = [zh[t, 0, ROWS * m : ROWS * m + ROWS] for m in range(bands // 2)]
        from_high = [zh[t, 1, ROWS * m : ROWS * m + ROWS] for m in range(bands // 2)]
        halos = {x: [[v[t, outside + 1, j, rows(k)] for k in range(bands)] for j in range(tiles)] for x, outside in edges}
        faces = []
        for k in range(bands):
            low, high = turned(from_low[k // 2], 1, 1), turned(from_high[k // 2], -1, 1)
            halo = jnp.where(even, low, high) if k % 2 == 0 else jnp.where(even, high, low)
            outer = blank
            for x, _ in edges:
                outer = packed(outer, x, k, halos[x][0][k], halos[x][-1][k])
            faces.append(partial[k] + wz[k] * (halo + outer))
        if t + 1 < SWEEPS:
            ship(t + 1, faces)
            start(z_copies(t + 1))
        for x, _ in edges:
            for k in range(bands):
                low = turned(from_low[k // 2], 1 - 2 * x - k % 2, 1)
                high = turned(from_high[k // 2], -1 - 2 * x - k % 2, 1)
                for j in range(tiles):
                    halo = halos[x][j][k]
                    if j == 0:
                        halo = halo + jnp.where(first_lane, low, 0.0)
                    if j == tiles - 1:
                        halo = halo + jnp.where(last_lane, high, 0.0)
                    new = get(t + 1, x, j, k) + w[x, j, ROWS * k : ROWS * k + ROWS] * halo
                    put(t + 1, x, j, k, new)
        if t + 1 < SWEEPS:
            start(x_copies(t + 1))
        mend(t + 1, faces)
        if t + 1 < SWEEPS:
            start(y_copies(t + 1))


def shards(initial, right_side, shift_field):
    nx, ny, nz = initial.shape
    assert nx % GROUP == 0 and nx % PREPARED == 0 and nx % CHUNKS == 0 and 2 * nx <= LANES
    assert ny % (2 * ROWS) == 0 and nz % LANES == 0
    faces, tiles = 2 * len(AXES), nz // LANES
    return pl.pallas_call(
        kernel,
        out_shape=pltpu.VMEM((nx, ny, nz), jnp.float32),
        in_specs=[pl.BlockSpec(memory_space=pltpu.HBM)] * 3,
        out_specs=pl.BlockSpec(memory_space=pltpu.VMEM),
        scratch_shapes=[
            pltpu.VMEM((SWEEPS, nx + 2, tiles, ny + 2 * ROWS, LANES), jnp.float32),
            pltpu.VMEM((nx, tiles, ny, LANES), jnp.float32),
            pltpu.VMEM((nx, tiles, ny, LANES), jnp.float32),
            pltpu.VMEM((SWEEPS, 2, ny // 2, LANES), jnp.float32),
            pltpu.VMEM((SWEEPS, 2, ny // 2, LANES), jnp.float32),
            pltpu.SemaphoreType.DMA(((CHUNKS + 2) * tiles,)),
            pltpu.SemaphoreType.DMA((SWEEPS, faces)),
            pltpu.SemaphoreType.DMA((SWEEPS, faces)),
        ],
        compiler_params=pltpu.CompilerParams(
            collective_id=0, has_side_effects=True, vmem_limit_bytes=40 * 1024 * 1024
        ),
    )(*(pltpu.with_memory_space_constraint(a, pltpu.HBM) for a in (initial, right_side, shift_field)))


def solution(mesh):
    spec = P(*AXES)
    return jax.shard_map(
        shards, mesh=mesh, in_specs=(spec, spec, spec), out_specs=spec, check_vma=False
    )
```

```python
import functools

import jax
import jax.numpy as jnp
import numpy as np
from jax import lax
from jax.experimental import pallas as pl
from jax.experimental.pallas import tpu as pltpu
from jax.sharding import PartitionSpec as P

SWEEPS = 4
PAIR = SWEEPS - 2
WEIGHT = np.float32(0.8)
KEEP = np.float32(1.0) - WEIGHT
AXES = ("gx", "gy", "gz")
MESH = pl.DeviceIdType.MESH
ROWS = 8
LANES = 128
GROUP = 32
PREPARED = 8
CHUNKS = 4


def beside(axis, step):
    count = lax.axis_size(axis)
    return {axis: lax.rem(lax.axis_index(axis) + (count + step), count)}


def across(x_step, z_step):
    return beside("gx", x_step) | beside("gz", z_step)


def iota(dim, shape):
    return lax.broadcasted_iota(jnp.int32, shape, dim)


def turned(block, shift, dim):
    size = block.shape[dim]
    shift = shift % size
    return block if shift == 0 else pltpu.roll(block, shift, dim)


def kernel(
    init_ref, rhs_ref, shift_ref, out_ref, v, q, w, z, zh, zd, wh, u, uh, wz_out, wzh, uz, uzh, load, send, recv, send2, recv2
):
    nx, ny, nz = out_ref.shape
    groups, bands, tiles = nx // GROUP, ny // ROWS, nz // LANES
    per = nx // CHUNKS

    barrier = pltpu.get_barrier_semaphore()
    for axis in AXES:
        for step in (-1, 1):
            pl.semaphore_signal(barrier, inc=1, device_id=beside(axis, step), device_id_type=MESH)

    def part(array, j):
        return array.at[:, :, pl.ds(LANES * j, LANES)]

    def init_copies(c):
        return [
            pltpu.make_async_copy(
                init_ref.at[pl.ds(c * per, per), :, pl.ds(LANES * j, LANES)],
                v.at[0, pl.ds(c * per + 1, per), j, pl.ds(ROWS, ny)],
                load.at[c * tiles + j],
            )
            for j in range(tiles)
        ]

    def field_copies(array, held, slot):
        return [
            pltpu.make_async_copy(part(array, j), held.at[:, j], load.at[(CHUNKS + slot) * tiles + j])
            for j in range(tiles)
        ]

    def start(copies):
        for copy in copies:
            copy.start()

    def wait(copies):
        for copy in copies:
            copy.wait()

    for c in range(CHUNKS):
        start(init_copies(c))
    field_loads = field_copies(shift_ref, w, 0) + field_copies(rhs_ref, q, 1)
    start(field_loads)

    def remote(src, dst, t, face, axis, step):
        return pltpu.make_async_remote_copy(
            src_ref=src,
            dst_ref=dst,
            send_sem=send.at[t, face],
            recv_sem=recv.at[t, face],
            device_id=beside(axis, step),
            device_id_type=MESH,
        )

    def x_copies(t):
        def plane(x):
            return v.at[t, x + 1, :, pl.ds(ROWS, ny)]

        return (
            remote(plane(nx - 1), plane(-1), t, 0, "gx", 1),
            remote(plane(0), plane(nx), t, 1, "gx", -1),
        )

    def y_copies(t):
        def row(y):
            return v.at[t, pl.ds(1, nx), :, pl.ds(ROWS + y, 1)]

        return (
            remote(row(ny - 1), row(-1), t, 2, "gy", 1),
            remote(row(0), row(ny), t, 3, "gy", -1),
        )

    def z_copies(t):
        return (
            remote(z.at[t, 1], zh.at[t, 0], t, 4, "gz", 1),
            remote(z.at[t, 0], zh.at[t, 1], t, 5, "gz", -1),
        )

    def later(src, dst, slot, place):
        return pltpu.make_async_remote_copy(
            src_ref=src,
            dst_ref=dst,
            send_sem=send2.at[slot],
            recv_sem=recv2.at[slot],
            device_id=place,
            device_id_type=MESH,
        )

    def weight_copies():
        return (
            later(w.at[nx - 1], wh.at[0], 0, beside("gx", 1)),
            later(w.at[0], wh.at[1], 1, beside("gx", -1)),
            later(wz_out.at[1], wzh.at[0], 2, beside("gz", 1)),
            later(wz_out.at[0], wzh.at[1], 3, beside("gz", -1)),
        )

    def sum_x_copies():
        return (
            later(u.at[1], uh.at[0], 4, beside("gx", 1)),
            later(u.at[0], uh.at[1], 5, beside("gx", -1)),
        )

    def sum_z_copies():
        return (
            later(uz.at[1], uzh.at[0], 6, beside("gz", 1)),
            later(uz.at[0], uzh.at[1], 7, beside("gz", -1)),
        )

    def corner_copies():
        return (
            later(z.at[PAIR, 1], zd.at[0, 0], 8, across(1, 1)),
            later(z.at[PAIR, 1], zd.at[0, 1], 9, across(-1, 1)),
            later(z.at[PAIR, 0], zd.at[1, 0], 10, across(1, -1)),
            later(z.at[PAIR, 0], zd.at[1, 1], 11, across(-1, -1)),
        )

    lane = iota(1, (ROWS, LANES))
    first_lane = lane == 0
    last_lane = lane == LANES - 1
    blank = jnp.zeros((ROWS, LANES), jnp.float32)

    def rows(k, shift=0):
        return slice(ROWS + ROWS * k + shift, 2 * ROWS + ROWS * k + shift)

    def packed(x, k, low, high):
        ends = jnp.where(first_lane, low, jnp.where(last_lane, high, 0.0))
        return turned(ends, 2 * x + k % 2, 1)

    even = lane % 2 == 0

    def ship(held, faces):
        for m in range(bands // 2):
            at = slice(ROWS * m, ROWS * m + ROWS)
            held[0, at] = jnp.where(even, faces[2 * m], faces[2 * m + 1])
            held[1, at] = jnp.where(even, faces[2 * m + 1], faces[2 * m])

    def put(t, x, j, k, new):
        if t < SWEEPS:
            v[t, x + 1, j, rows(k)] = new
        else:
            out_ref[x, ROWS * k : ROWS * k + ROWS, LANES * j : LANES * j + LANES] = new

    def get(t, x, j, k):
        if t < SWEEPS:
            return v[t, x + 1, j, rows(k)]
        return out_ref[x, ROWS * k : ROWS * k + ROWS, LANES * j : LANES * j + LANES]

    def put_lane(t, x, j, k, new, mask):
        if t < SWEEPS:
            pltpu.store(v.at[t, x + 1, j, pl.ds(ROWS + ROWS * k, ROWS)], new, mask=mask)
        else:
            pltpu.store(
                out_ref.at[x, pl.ds(ROWS * k, ROWS), pl.ds(LANES * j, LANES)], new, mask=mask
            )

    def packed_all(low, high, ks):
        faces = {}
        for k in ks:
            sums = [packed(x, k, low(x, k), high(x, k)) for x in range(nx)]
            while len(sums) > 1:
                sums = [a + b for a, b in zip(sums[0::2], sums[1::2])] + sums[len(sums) // 2 * 2 :]
            faces[k] = sums[0]
        return faces

    for c in range(CHUNKS):
        wait(init_copies(c))
    face = packed_all(lambda x, k: v[0, x + 1, 0, rows(k)], lambda x, k: v[0, x + 1, tiles - 1, rows(k)], range(bands))
    ship(z.at[0], face)

    pl.semaphore_wait(barrier, 2 * len(AXES))
    start(z_copies(0) + x_copies(0) + y_copies(0))

    wait(field_loads)

    def prepare(g, carry):
        for i in range(PREPARED):
            x = g * PREPARED + i
            for k in range(bands):
                at = slice(ROWS * k, ROWS * k + ROWS)
                for j in range(tiles):
                    ratio = WEIGHT / (6.0 + w[x, j, at])
                    w[x, j, at] = ratio
                    q[x, j, at] = ratio * q[x, j, at]
        return carry

    lax.fori_loop(0, nx // PREPARED, prepare, 0)
    wz = packed_all(
        lambda x, k: w[x, 0, ROWS * k : ROWS * k + ROWS],
        lambda x, k: w[x, tiles - 1, ROWS * k : ROWS * k + ROWS],
        range(bands),
    )
    ship(wz_out, wz)
    start(weight_copies())

    def bulk_group(t, ks, g, carry):
        base = g * GROUP
        seen = {}

        def plane(i):
            if i not in seen:
                x = base + i
                if i < 0:
                    x = jnp.maximum(x, 0)
                if i == GROUP:
                    x = jnp.minimum(x, nx - 1)
                seen[i] = [{k: v[t, x + 1, j, rows(k)] for k in ks} for j in range(tiles)]
                if i < 0:
                    inside = jnp.where(g > 0, 1.0, 0.0)
                    seen[i] = [{k: inside * column[k] for k in ks} for column in seen[i]]
                if i == GROUP:
                    inside = jnp.where(g < groups - 1, 1.0, 0.0)
                    seen[i] = [{k: inside * column[k] for k in ks} for column in seen[i]]
            return seen[i]

        for i in range(GROUP):
            x = base + i
            centre, below, above = plane(i), plane(i - 1), plane(i + 1)
            for k in ks:
                at = slice(ROWS * k, ROWS * k + ROWS)
                before = [turned(centre[j][k], 1, 1) for j in range(tiles)]
                after = [turned(centre[j][k], -1, 1) for j in range(tiles)]
                for j in range(tiles):
                    total = v[t, x + 1, j, rows(k, -1)] + v[t, x + 1, j, rows(k, 1)]
                    total = total + (below[j][k] + above[j][k])
                    low = before[j - 1] if j else 0.0
                    high = after[j + 1] if j + 1 < tiles else 0.0
                    total = total + (
                        jnp.where(first_lane, low, before[j]) + jnp.where(last_lane, high, after[j])
                    )
                    put(t + 1, x, j, k, (KEEP * centre[j][k] + q[x, j, at]) + w[x, j, at] * total)
        return carry

    def bulk(t, ks):
        lax.fori_loop(0, groups, functools.partial(bulk_group, t, ks), 0)

    def mend(t, faces, ks):
        for x in range(1, nx - 1):
            for k in ks:
                value = turned(faces[k], -2 * x - k % 2, 1)
                put_lane(t, x, 0, k, value, first_lane)
                put_lane(t, x, tiles - 1, k, value, last_lane)

    edges = ((0, -1), (nx - 1, nx))
    inner, outer = tuple(range(1, bands - 1)), tuple(sorted({0, bands - 1}))

    def halves(held):
        return [held[ROWS * m : ROWS * m + ROWS] for m in range(bands // 2)]

    def beyond(low, high, x):
        cells = {}
        for k in range(bands):
            if tiles > 1:
                for j in range(1, tiles - 1):
                    cells[j, k] = 0.0
            cells[0, k] = jnp.where(first_lane, turned(low[k // 2], 1 - 2 * x - k % 2, 1), 0.0)
            last = jnp.where(last_lane, turned(high[k // 2], -1 - 2 * x - k % 2, 1), 0.0)
            cells[tiles - 1, k] = last if tiles > 1 else cells[0, k] + last
        return cells

    def received(t):
        halos = {
            x: {(j, k): v[t, outside + 1, j, rows(k)] for j in range(tiles) for k in range(bands)} for x, outside in edges
        }
        return halos, halves(zh.at[t, 0]), halves(zh.at[t, 1])

    def worked_out(t):
        halos = {}
        for side, (x, _) in enumerate(edges):
            there = nx - 1 if side == 0 else 0
            cells = beyond(halves(zd.at[0, side]), halves(zd.at[1, side]), there)
            halos[x] = {}
            for j in range(tiles):
                for k in range(bands):
                    at = slice(ROWS * k, ROWS * k + ROWS)
                    total = v[t, x + 1, j, rows(k)] + cells[j, k]
                    halos[x][j, k] = uh[side, j, at] + wh[side, j, at] * total
        packs = []
        for face in range(2):
            turn = 1 if face else -1
            own = halves(z.at[t, 1 if face else 0])
            below, above = halves(zd.at[face, 0]), halves(zd.at[face, 1])
            sums, weights = halves(uzh.at[face]), halves(wzh.at[face])
            pack = []
            for m in range(bands // 2):
                total = turned(own[m], turn, 1)
                start_lane = 0 if face else LANES - 1
                at_first = (lane == start_lane) | (lane == (start_lane + 1) % LANES)
                end_lane = (start_lane + 2 * (nx - 1)) % LANES
                at_last = (lane == end_lane) | (lane == (end_lane + 1) % LANES)
                total = total + jnp.where(at_first, turned(below[m], -2 * (nx - 1), 1), 0.0)
                total = total + jnp.where(at_last, turned(above[m], 2 * (nx - 1), 1), 0.0)
                pack.append(sums[m] + weights[m] * total)
            packs.append(pack)
        return halos, packs[0], packs[1]

    for t in range(SWEEPS):
        def summed(ks):
            bulk(t, ks)
            return packed_all(lambda x, k: get(t + 1, x, 0, k), lambda x, k: get(t + 1, x, tiles - 1, k), ks)

        partial = summed(inner) if inner else {}
        wait(y_copies(t))
        partial |= summed(outer)
        if t == PAIR:
            for side, (x, _) in enumerate(edges):
                for j in range(tiles):
                    u[side, j] = v[t + 1, x + 1, j, ROWS : ROWS + ny]
            start(sum_x_copies())
        if t == PAIR:
            ship(uz, partial)
            start(sum_z_copies())
        if t == PAIR + 1:
            wait(sum_x_copies() + sum_z_copies() + corner_copies() + weight_copies())
            halos, from_low, from_high = worked_out(PAIR)
        else:
            wait(x_copies(t) + z_copies(t))
            halos, from_low, from_high = received(t)
        sends = t + 1 < SWEEPS and t != PAIR
        faces = []
        for k in range(bands):
            low, high = turned(from_low[k // 2], 1, 1), turned(from_high[k // 2], -1, 1)
            halo = jnp.where(even, low, high) if k % 2 == 0 else jnp.where(even, high, low)
            aside = blank
            for x, _ in edges:
                aside = aside + packed(x, k, halos[x][0, k], halos[x][tiles - 1, k])
            faces.append(partial[k] + wz[k] * (halo + aside))
        if sends:
            ship(z.at[t + 1], faces)
            start(z_copies(t + 1))
            if t + 1 == PAIR:
                start(corner_copies())
        for x, _ in edges:
            cells = beyond(from_low, from_high, x)
            for j in range(tiles):
                for k in range(bands):
                    new = get(t + 1, x, j, k) + w[x, j, ROWS * k : ROWS * k + ROWS] * (halos[x][j, k] + cells[j, k])
                    put(t + 1, x, j, k, new)
        if sends:
            start(x_copies(t + 1))
        mend(t + 1, faces, outer)
        if t + 1 < SWEEPS:
            start(y_copies(t + 1))
        mend(t + 1, faces, inner)


def shards(initial, right_side, shift_field):
    nx, ny, nz = initial.shape
    assert nx % GROUP == 0 and nx % PREPARED == 0 and nx % CHUNKS == 0 and 2 * nx <= LANES
    assert ny % (2 * ROWS) == 0 and nz % LANES == 0
    faces, tiles = 2 * len(AXES), nz // LANES
    return pl.pallas_call(
        kernel,
        out_shape=pltpu.VMEM((nx, ny, nz), jnp.float32),
        in_specs=[pl.BlockSpec(memory_space=pltpu.HBM)] * 3,
        out_specs=pl.BlockSpec(memory_space=pltpu.VMEM),
        scratch_shapes=[
            pltpu.VMEM((SWEEPS, nx + 2, tiles, ny + 2 * ROWS, LANES), jnp.float32),
            pltpu.VMEM((nx, tiles, ny, LANES), jnp.float32),
            pltpu.VMEM((nx, tiles, ny, LANES), jnp.float32),
            pltpu.VMEM((SWEEPS, 2, ny // 2, LANES), jnp.float32),
            pltpu.VMEM((SWEEPS, 2, ny // 2, LANES), jnp.float32),
            pltpu.VMEM((2, 2, ny // 2, LANES), jnp.float32),
            pltpu.VMEM((2, tiles, ny, LANES), jnp.float32),
            pltpu.VMEM((2, tiles, ny, LANES), jnp.float32),
            pltpu.VMEM((2, tiles, ny, LANES), jnp.float32),
            pltpu.VMEM((2, ny // 2, LANES), jnp.float32),
            pltpu.VMEM((2, ny // 2, LANES), jnp.float32),
            pltpu.VMEM((2, ny // 2, LANES), jnp.float32),
            pltpu.VMEM((2, ny // 2, LANES), jnp.float32),
            pltpu.SemaphoreType.DMA(((CHUNKS + 2) * tiles,)),
            pltpu.SemaphoreType.DMA((SWEEPS, faces)),
            pltpu.SemaphoreType.DMA((SWEEPS, faces)),
            pltpu.SemaphoreType.DMA((12,)),
            pltpu.SemaphoreType.DMA((12,)),
        ],
        compiler_params=pltpu.CompilerParams(
            collective_id=0, has_side_effects=True, vmem_limit_bytes=40 * 1024 * 1024
        ),
    )(*(pltpu.with_memory_space_constraint(a, pltpu.HBM) for a in (initial, right_side, shift_field)))


def solution(mesh):
    spec = P(*AXES)
    return jax.shard_map(
        shards, mesh=mesh, in_specs=(spec, spec, spec), out_specs=spec, check_vma=False
    )
```
